32 devices in a mesh: dp: 4 (over y, x), cp: 8 (over z, core).
Axes of the slice: x: 2, y: 2, z: 4, core: 2. Of those that a mesh axis runs over, the one named last changes fastest.
Arguments:
- tokens: bfloat16 [4, 1024, 4096], P('dp', 'cp'), may hold values from -60 to 60
- qkv_weight: bfloat16 [4096, 3072], replicated, may hold values from -0.09375 to 0.09375
- owner_slot: int32 [4, 8], P('dp', 'cp'), may hold values from 0 to 3, as said below
- slab_sequence: int32 [4, 8], replicated, may hold values from 0 to 4, as said below
- slab_order: int32 [4, 8], replicated, may hold values from 0 to 3, as said below
Outputs:
- context: bfloat16 [4, 1024, 2048], P('dp', 'cp')
The draws below stay inside these ranges and needn't reach their ends.
Inputs may be any that keep to these rules, and one draw needn't show every extreme that they name: For every column c, the entries owner_slot[a, c] over all rows a are 0 to 3, each once. `slab_sequence`: in each row, the slabs with one sequence number carry the orders 0 to L-1, each once, L being their count; no sequence has more than 4 slabs. `slab_order`: see slab_sequence.
All inputs are finite; a program needn't handle non-finite values.
Results may differ from the reference program's by a relative error of at most 0.006.
The reference program's roundings to bfloat16 on the way count: a program that leaves them out, or rounds other values in their place, can miss the bound.
Values may be sent and summed in bfloat16 or wider, within the bound.
A program may use at most 128 MiB of HBM per device.

```python
import jax
import jax.numpy as jnp
from jax import lax

D = 4096
QH = 16
KVH = 4
HD = 128
SLAB = 128
SLABS_DEV = 1
GROUPS = 4
ROW_SLABS = 8
ROW_TOK = 1024


def sequence_plan(key):
    half_count = ROW_SLABS // 2
    chosen_row = jax.random.randint(jax.random.fold_in(key, 9), (), 0, GROUPS)
    singles_flags = jnp.arange(GROUPS, dtype=jnp.int32) == chosen_row

    def one_row(row_key, singles):
        first_key, second_key = jax.random.split(row_key)
        index = jnp.arange(ROW_SLABS, dtype=jnp.int32)
        random_starts = jax.random.randint(first_key, (ROW_SLABS,), 0, 8) == 0
        later_starts = random_starts | (index == half_count) | singles
        starts = jnp.where(index < half_count, index == 0, later_starts)
        numbers = jnp.cumsum(starts.astype(jnp.int32)) - 1
        begins = lax.cummax(jnp.where(starts, index, 0))
        shuffle = jax.random.permutation(second_key, ROW_SLABS)
        return (numbers[shuffle].astype(jnp.int32), (index - begins)[shuffle].astype(jnp.int32))
    return jax.vmap(one_row)(jax.random.split(jax.random.fold_in(key, 7), GROUPS), singles_flags)


def draw_slab_sequence(key, part):
    return sequence_plan(key)[0]


def draw_slab_order(key, part):
    return sequence_plan(key)[1]


def draw_owner_slot(key, part):
    columns_count = ROW_SLABS // SLABS_DEV
    column_keys = jax.random.split(jax.random.fold_in(key, 3), columns_count)

    def one_column(column_key):
        return jax.random.permutation(column_key, GROUPS * SLABS_DEV).astype(jnp.int32).reshape(GROUPS, SLABS_DEV)
    stacked = jax.vmap(one_column)(column_keys)
    return stacked.transpose(1, 0, 2).reshape(GROUPS, ROW_SLABS)


def draw_tokens(key, part):
    first_key, second_key = jax.random.split(jax.random.fold_in(key, 11))
    values = jax.random.normal(first_key, (GROUPS, ROW_TOK, D), jnp.float32)
    values = jnp.clip(values, -6.0, 6.0)
    return values.astype(jnp.bfloat16)


def scatter_about(stream_key, extent, spread, most, kind=jnp.bfloat16):
    drawn = jax.random.normal(stream_key, extent, jnp.float32) * spread
    return jnp.minimum(jnp.maximum(drawn, -most), most).astype(kind)


def setup_inputs(seed: int = 0) -> dict:
    key_of = jax.random.split(jax.random.key(seed), 6)
    tokens = draw_tokens(jax.random.fold_in(key_of[5], 71), 0)
    qkv_weight = scatter_about(key_of[1], (D, (QH + 2 * KVH) * HD), D ** -0.5, 0.09375)
    owner_slot = draw_owner_slot(jax.random.fold_in(key_of[5], 71), 0)
    slab_sequence = draw_slab_sequence(jax.random.fold_in(key_of[5], 71), 0)
    slab_order = draw_slab_order(jax.random.fold_in(key_of[5], 71), 0)
    return dict(tokens=tokens, qkv_weight=qkv_weight, owner_slot=owner_slot, slab_sequence=slab_sequence, slab_order=slab_order)


ROPE_BASE = 500000.0
NEG_FILL = -1e30


def rotate(heads, positions):
    half_dim = heads.shape[-1] // 2
    frequency = ROPE_BASE ** (-jnp.arange(half_dim, dtype=jnp.float32) * 2.0 / heads.shape[-1])
    angles = positions.astype(jnp.float32)[:, None] * frequency[None, :]
    cosine = jnp.cos(angles)[:, None, :]
    sine_part = jnp.sin(angles)[:, None, :]
    first_half = heads[..., :half_dim]
    second_half = heads[..., half_dim:]
    return jnp.concatenate([first_half * cosine - second_half * sine_part, second_half * cosine + first_half * sine_part], axis=-1)


def project(input_rows, weight, positions):
    projected = jnp.dot(input_rows, weight, preferred_element_type=jnp.float32)
    count_rows = input_rows.shape[0]
    query = rotate(projected[:, :QH * HD].reshape(count_rows, QH, HD), positions).astype(jnp.bfloat16)
    key_heads = rotate(projected[:, QH * HD:(QH + KVH) * HD].reshape(count_rows, KVH, HD), positions).astype(jnp.bfloat16)
    value_heads = projected[:, (QH + KVH) * HD:].astype(jnp.bfloat16)
    key_value = jnp.concatenate([key_heads.reshape(count_rows, KVH * HD), value_heads], axis=1)
    return query.reshape(count_rows, QH * HD), key_value


def attend(query, key_value, query_pos, query_code, key_code):
    count_rows = query.shape[0]
    block_rows = min(512, count_rows)
    group_size = QH // KVH
    keys_f = key_value[:, :KVH * HD].reshape(-1, KVH, HD).astype(jnp.float32)
    values_f = key_value[:, KVH * HD:].reshape(-1, KVH, HD).astype(jnp.float32)

    def per_block(args):
        query_block, pos_block, code_block = args
        query_f = query_block.reshape(block_rows, KVH, group_size, HD).astype(jnp.float32)
        scores = jnp.einsum('tgjh,ngh->gjtn', query_f, keys_f) * (HD ** -0.5)
        allowed = (key_code[None, :] <= code_block[:, None]) & (key_code[None, :] >= (code_block - pos_block)[:, None])
        scores = jnp.where(allowed, scores, NEG_FILL)
        row_max = jnp.max(scores, axis=-1, keepdims=True)
        weights = jnp.where(allowed, jnp.exp(scores - row_max), 0.0)
        denom_sum = jnp.sum(weights, axis=-1)
        rounded = lax.optimization_barrier(weights.astype(jnp.bfloat16))
        weighted = jnp.einsum('gjtn,ngh->gjth', rounded.astype(jnp.float32), values_f)
        context = weighted / denom_sum[..., None]
        return context.transpose(2, 0, 1, 3).reshape(block_rows, QH * HD).astype(jnp.bfloat16)

    blocks = count_rows // block_rows
    result = lax.map(per_block, (query.reshape(blocks, block_rows, QH * HD), query_pos.reshape(blocks, block_rows), query_code.reshape(blocks, block_rows)))
    return result.reshape(count_rows, QH * HD)


def reference(tokens, qkv_weight, owner_slot, slab_sequence, slab_order):
    columns_count = ROW_SLABS // SLABS_DEV
    slabs = tokens.reshape(GROUPS, columns_count, SLABS_DEV, SLAB, D)
    targets = owner_slot.reshape(GROUPS, columns_count, SLABS_DEV)
    columns = jnp.broadcast_to(jnp.arange(columns_count, dtype=jnp.int32)[None, :, None], targets.shape)
    owner_rows = jnp.zeros_like(slabs).at[targets // SLABS_DEV, columns, targets % SLABS_DEV].set(slabs)
    owner_rows = owner_rows.reshape(GROUPS, ROW_TOK, D)
    offsets = jnp.arange(SLAB, dtype=jnp.int32)
    positions = (slab_order[:, :, None] * SLAB + offsets[None, None, :]).reshape(GROUPS, ROW_TOK)
    codes = (slab_sequence[:, :, None] * ROW_TOK).reshape(GROUPS, ROW_SLABS, 1) + positions.reshape(GROUPS, ROW_SLABS, SLAB)
    codes = codes.reshape(GROUPS, ROW_TOK).astype(jnp.int32)

    def per_row(args):
        input_rows, row_pos, row_code = args
        query, key_value = project(input_rows, qkv_weight, row_pos)
        return attend(query, key_value, row_pos, row_code, row_code)

    return lax.map(per_row, (owner_rows, positions, codes))
```

```python
import functools

import jax
import jax.numpy as jnp
from jax import lax
from jax.experimental import pallas as pl
from jax.experimental.pallas import tpu as pltpu
from jax.sharding import PartitionSpec as P

QH = 16
KVH = 4
HD = 128
ROPE_BASE = 500000.0
NEG_FILL = -1e30
MESH = pl.DeviceIdType.MESH
UNIT = 2 * HD
AHEAD = 5


def schedule(nz):
    zs = sorted(
        ((g, d) for d in range(1, nz) for g in range(KVH)), key=lambda e: (e[0] + 2 * (e[1] - 1), e[1])
    )
    zs = [("Z", g, d) for g, d in zs]
    steps = []

    def add(text):
        for word in text.split():
            if word == "Z":
                if zs:
                    steps.append(zs.pop(0))
                continue
            kind, number = word[0], int(word[1:])
            if kind == "Q":
                steps.extend([("P", number), ("S", number)])
            else:
                steps.append((kind, number))

    for text in (
        "Q0 Q1 Q2 Q3",
        "T0 T1 P4 T2",
        "T3 S4 Q5",
        "F0 F1 Q6 F2",
        "F3 Q7 Q8 Z",
        "Q9 Z T4 T5",
        "Q10 Z T6 T7",
        "Q11 Z F4 F5",
        "T8 T9 Z F6",
        "F7 T10 T11 Z",
        "F8 F9 Z F10",
        "F11",
    ):
        add(text)
    for entry in zs:
        steps.append(entry)
        if entry[2] == nz - 1:
            steps.append(("A", entry[1]))
    done = {e[1] for e in steps if e[0] == "A"}
    steps.extend(("A", g) for g in range(KVH) if g not in done)
    return steps


def kernel(
    groups, columns, seq_ref, order_ref, slot_ref, cos_ref, sin_ref, x_hbm, w_hbm, out_ref,
    x_ref, w_ref, own, recv1, send2, recv2, query, kv0, kv1, kv2, kv3, t_own, t_a, t_b,
    x_sem, w_sem, s1_send, s1_recv, s2_send, s2_recv, t_send, t_recv,
    left_send, right_send, core_send, z_recv, core_recv,
):
    kvs = (kv0, kv1, kv2, kv3)
    rows = out_ref.shape[0]
    units = w_ref.shape[0]
    nz = columns // 2
    me = lax.axis_index("dp")
    cp = lax.axis_index("cp")
    z = cp // 2
    core = cp % 2
    near = {1: me + 1 - 2 * (me % 2), 2: (me + 2) % groups}
    partner = (me, cp + 1 - 2 * core)

    def weight_copies(u):
        if u < KVH:
            k_col = QH * HD + u * HD
            v_col = (QH + KVH) * HD + u * HD
            return [
                pltpu.make_async_copy(
                    w_hbm.at[:, pl.ds(k_col, HD)], w_ref.at[u, :, pl.ds(0, HD)], w_sem.at[u, 0]
                ),
                pltpu.make_async_copy(
                    w_hbm.at[:, pl.ds(v_col, HD)], w_ref.at[u, :, pl.ds(HD, HD)], w_sem.at[u, 1]
                ),
            ]
        return [
            pltpu.make_async_copy(
                w_hbm.at[:, pl.ds((u - KVH) * UNIT, UNIT)], w_ref.at[u], w_sem.at[u, 0]
            )
        ]

    x_copy = pltpu.make_async_copy(x_hbm, x_ref, x_sem)
    x_copy.start()
    for u in range(AHEAD):
        for copy in weight_copies(u):
            copy.start()

    barrier = pltpu.get_barrier_semaphore()

    def greet(device):
        pl.semaphore_signal(barrier, inc=1, device_id=device, device_id_type=MESH)

    greet((near[1], cp))
    greet((near[2], cp))
    greet(partner)
    has_left = z > 0
    has_right = z < nz - 1
    pl.when(has_left)(lambda: greet((me, cp - 2)))
    pl.when(has_right)(lambda: greet((me, cp + 2)))

    target = slot_ref[0, 0]
    t_own[...] = jnp.full(t_own.shape, target, jnp.int32)

    own_seq = seq_ref[me, cp]
    own_order = order_ref[me, cp]
    most = columns // 2
    table = []
    for i in range(most):
        index = cp
        for s in range(columns):
            hit = (seq_ref[me, s] == own_seq) & (order_ref[me, s] == i)
            index = jnp.where(hit, s, index)
        table.append(index)

    def first_bit(u):
        return 1 if u % 2 == 0 else 2

    def remote(src, dst, send, recv, device):
        return pltpu.make_async_remote_copy(
            src_ref=src, dst_ref=dst, send_sem=send, recv_sem=recv, device_id=device, device_id_type=MESH
        )

    def t_copy(bit):
        return remote(
            t_own, t_a if bit == 1 else t_b, t_send.at[bit - 1], t_recv.at[bit - 1], (near[bit], cp)
        )

    def hop1(u):
        return remote(own.at[u], recv1.at[u], s1_send.at[u], s1_recv.at[u], (near[first_bit(u)], cp))

    def hop2(u):
        return remote(
            send2.at[u], recv2.at[u], s2_send.at[u], s2_recv.at[u], (near[3 - first_bit(u)], cp)
        )

    def left_copy(g, zs):
        block = kvs[g].at[2 * zs + core]
        return remote(block, block, left_send.at[g, zs], z_recv.at[g, zs], (me, cp - 2))

    def right_copy(g, zs):
        block = kvs[g].at[2 * zs + core]
        return remote(block, block, right_send.at[g, zs], z_recv.at[g, zs], (me, cp + 2))

    def core_copy(g, zs):
        block = kvs[g].at[2 * zs + core]
        return remote(block, block, core_send.at[g, zs], core_recv.at[g, zs], partner)

    def project(u):
        for copy in weight_copies(u):
            copy.wait()
        if u + AHEAD < units:
            for copy in weight_copies(u + AHEAD):
                copy.start()
        product = jnp.dot(x_ref[...], w_ref[u], preferred_element_type=jnp.float32)
        for half in range(2):
            part = product[:, half * HD : (half + 1) * HD]
            if not (u < KVH and half == 1):
                part = part * cos_ref[...] + pltpu.roll(part, HD // 2, 1) * sin_ref[...]
            own[u, :, pl.ds(half * HD, HD)] = part.astype(jnp.bfloat16)

    def is_target(ref, device):
        return jnp.broadcast_to(ref[0:1, :] == device, (rows, HD))

    def halves(ref, u):
        return [ref[u, :, pl.ds(h * HD, HD)].astype(jnp.float32) for h in range(2)]

    def second(u):
        hop1(u).wait_recv()
        passes = is_target(t_own, near[3 - first_bit(u)])
        mine, came = halves(own, u), halves(recv1, u)
        for h in range(2):
            send2[u, :, pl.ds(h * HD, HD)] = jnp.where(passes, mine[h], came[h]).astype(jnp.bfloat16)
        hop2(u).start()

    def arrive(u):
        hop2(u).wait_recv()
        stays = is_target(t_own, me)
        first = is_target(t_a if first_bit(u) == 1 else t_b, me)
        mine, came1, came2 = halves(own, u), halves(recv1, u), halves(recv2, u)
        for h in range(2):
            value = jnp.where(stays, mine[h], jnp.where(first, came1[h], came2[h])).astype(jnp.bfloat16)
            if u < KVH:
                kvs[u][cp, :, pl.ds(h * HD, HD)] = value
            else:
                query[2 * (u - KVH) + h] = value
        if u < KVH:
            pl.when(has_left)(lambda: left_copy(u, z).start())
            pl.when(has_right)(lambda: right_copy(u, z).start())
            core_copy(u, z).start()

    def along(g, d):
        @pl.when(z + d < nz)
        def _():
            left_copy(g, z + d).wait_recv()
            pl.when(has_left)(lambda: left_copy(g, z + d).start())
            core_copy(g, z + d).start()

        @pl.when(z - d >= 0)
        def _():
            right_copy(g, z - d).wait_recv()
            pl.when(has_right)(lambda: right_copy(g, z - d).start())
            core_copy(g, z - d).start()

    def attend(g):
        for zs in range(nz):
            core_copy(g, zs).wait_recv()
        blocks = [kvs[g][index] for index in table]
        keys = jnp.concatenate([b[:, :HD] for b in blocks], axis=0)
        values = jnp.concatenate([b[:, HD:] for b in blocks], axis=0)
        shape = (rows, keys.shape[0])
        row_pos = lax.broadcasted_iota(jnp.int32, shape, 0) + own_order * rows
        allowed = lax.broadcasted_iota(jnp.int32, shape, 1) <= row_pos
        for j in range(QH // KVH):
            head = g * (QH // KVH) + j
            scores = lax.dot_general(
                query[head], keys, (((1,), (1,)), ((), ())), preferred_element_type=jnp.float32
            )
            scores = jnp.where(allowed, scores * (HD ** -0.5), NEG_FILL)
            peak = jnp.max(scores, axis=1, keepdims=True)
            weights = jnp.exp(scores - peak)
            total = jnp.sum(weights, axis=1, keepdims=True)
            mixed = jnp.dot(weights.astype(jnp.bfloat16), values, preferred_element_type=jnp.float32)
            out_ref[:, pl.ds(head * HD, HD)] = (mixed / total).astype(jnp.bfloat16)

    x_copy.wait()
    for step in schedule(nz):
        kind, u = step[0], step[1]
        if kind == "P":
            project(u)
        elif kind == "S":
            if u == 0:
                pl.semaphore_wait(barrier, 3 + jnp.minimum(z, 1) + jnp.minimum(nz - 1 - z, 1))
                t_copy(1).start()
                t_copy(2).start()
            hop1(u).start()
        elif kind == "T":
            if u == 0:
                t_copy(1).wait()
                t_copy(2).wait()
            second(u)
        elif kind == "F":
            arrive(u)
        elif kind == "Z":
            along(u, step[2])
        else:
            attend(u)

    for u in range(units):
        hop1(u).wait_send()
        hop2(u).wait_send()
    for g in range(KVH):
        for zs in range(nz):
            core_copy(g, zs).wait_send()

            @pl.when(has_left & (z <= zs))
            def _():
                left_copy(g, zs).wait_send()

            @pl.when(has_right & (z >= zs))
            def _():
                right_copy(g, zs).wait_send()


def local(tokens, qkv_weight, owner_slot, slab_sequence, slab_order):
    loader_rows = tokens[0]
    rows, width = loader_rows.shape
    groups = lax.axis_size("dp")
    columns = lax.axis_size("cp")
    assert groups == 4 and columns % 2 == 0 and owner_slot.shape[1] == 1
    assert slab_sequence.shape[1] == columns
    nz = columns // 2
    units = (QH + 2 * KVH) * HD // UNIT
    sent_order = slab_order[owner_slot[0, 0], lax.axis_index("cp")]
    positions = (sent_order * rows + jnp.arange(rows, dtype=jnp.int32)).astype(jnp.float32)
    half = HD // 2
    frequency = ROPE_BASE ** (-jnp.arange(half, dtype=jnp.float32) * 2.0 / HD)
    angles = positions[:, None] * frequency[None, :]
    cosine, sine = jnp.cos(angles), jnp.sin(angles)
    cos_table = jnp.concatenate([cosine, cosine], axis=1)
    sin_table = jnp.concatenate([-sine, sine], axis=1)
    smem = pl.BlockSpec(memory_space=pltpu.SMEM)
    vmem = pl.BlockSpec(memory_space=pltpu.VMEM)
    hbm = pl.BlockSpec(memory_space=pl.ANY)
    unit_buffer = pltpu.VMEM((units, rows, UNIT), jnp.bfloat16)
    kv_buffer = pltpu.VMEM((columns, rows, UNIT), jnp.bfloat16)
    small = pltpu.VMEM((8, HD), jnp.int32)
    dma = pltpu.SemaphoreType.DMA
    context = pl.pallas_call(
        functools.partial(kernel, groups, columns),
        out_shape=jax.ShapeDtypeStruct((rows, QH * HD), jnp.bfloat16),
        in_specs=[smem, smem, smem, vmem, vmem, hbm, hbm],
        out_specs=vmem,
        scratch_shapes=[
            pltpu.VMEM((rows, width), jnp.bfloat16),
            pltpu.VMEM((units, width, UNIT), jnp.bfloat16),
            unit_buffer,
            unit_buffer,
            unit_buffer,
            unit_buffer,
            pltpu.VMEM((QH, rows, HD), jnp.bfloat16),
            kv_buffer,
            kv_buffer,
            kv_buffer,
            kv_buffer,
            small,
            small,
            small,
            dma,
            dma((units, 2)),
            dma((units,)),
            dma((units,)),
            dma((units,)),
            dma((units,)),
            dma((2,)),
            dma((2,)),
            dma((KVH, nz)),
            dma((KVH, nz)),
            dma((KVH, nz)),
            dma((KVH, nz)),
            dma((KVH, nz)),
        ],
        compiler_params=pltpu.CompilerParams(
            collective_id=0, has_side_effects=True, vmem_limit_bytes=60000 * 1024
        ),
    )(slab_sequence, slab_order, owner_slot, cos_table, sin_table, loader_rows, qkv_weight)
    return context[None]


def solution(mesh):
    in_specs = (P("dp", "cp", None), P(), P("dp", "cp"), P(), P())
    out_specs = P("dp", "cp", None)
    return jax.shard_map(local, mesh=mesh, in_specs=in_specs, out_specs=out_specs, check_vma=False)
```

```python
import functools

import jax
import jax.numpy as jnp
import numpy as np
from jax import lax
from jax.experimental import pallas as pl
from jax.experimental.pallas import tpu as pltpu
from jax.sharding import PartitionSpec as P

QH = 16
KVH = 4
HD = 128
ROPE_BASE = 500000.0
NEG_FILL = -1e30
MESH = pl.DeviceIdType.MESH
UNIT = 2 * HD
AHEAD = 2


def schedule(nz):
    zs = sorted(
        ((g, d) for d in range(1, nz) for g in range(KVH)), key=lambda e: (e[0] + 2 * (e[1] - 1), e[1])
    )
    zs = [("Z", g, d) for g, d in zs]
    steps = []

    def add(text):
        for word in text.split():
            if word == "Z":
                if zs:
                    steps.append(zs.pop(0))
                continue
            kind, number = word[0], int(word[1:])
            if kind == "Q":
                steps.extend([("P", number), ("S", number)])
            else:
                steps.append((kind, number))

    for text in (
        "Q0 Q1 Q2 Q3",
        "T0 T1 P4 T2",
        "T3 S4 Q5 F0",
        "F1 Q6 F2 F3",
        "Q7 Q8 Z Q9",
        "Z T4 T5 Q10",
        "Z T6 T7 Q11",
        "Z F4 F5 T8",
        "T9 Z F6 F7",
        "T10 T11 Z F8",
        "F9 Z F10 F11",
    ):
        add(text)
    for entry in zs:
        steps.append(entry)
        if entry[2] == nz - 1:
            steps.append(("A", entry[1]))
    done = {e[1] for e in steps if e[0] == "A"}
    steps.extend(("A", g) for g in range(KVH) if g not in done)
    return steps


def kernel(
    groups, columns, seq_ref, order_ref, slot_ref, start_ref, offset_ref, sign_ref, x_hbm, w_hbm, out_ref,
    x_ref, w_ref, own, recv1, send2, recv2, query, kv0, kv1, kv2, kv3, t_own, t_a, t_b, cos_ref, sin_ref,
    x_sem, w_sem, s1_send, s1_recv, s2_send, s2_recv, t_send, t_recv,
    left_send, right_send, core_send, z_recv, core_recv,
):
    kvs = (kv0, kv1, kv2, kv3)
    rows = out_ref.shape[0]
    units = w_ref.shape[0]
    nz = columns // 2
    me = lax.axis_index("dp")
    cp = lax.axis_index("cp")
    z = cp // 2
    core = cp % 2
    near = {1: me + 1 - 2 * (me % 2), 2: (me + 2) % groups}
    partner = (me, cp + 1 - 2 * core)

    def weight_copies(u):
        if u < KVH:
            k_col = QH * HD + u * HD
            v_col = (QH + KVH) * HD + u * HD
            return [
                pltpu.make_async_copy(
                    w_hbm.at[:, pl.ds(k_col, HD)], w_ref.at[u, :, pl.ds(0, HD)], w_sem.at[u, 0]
                ),
                pltpu.make_async_copy(
                    w_hbm.at[:, pl.ds(v_col, HD)], w_ref.at[u, :, pl.ds(HD, HD)], w_sem.at[u, 1]
                ),
            ]
        return [
            pltpu.make_async_copy(
                w_hbm.at[:, pl.ds((u - KVH) * UNIT, UNIT)], w_ref.at[u], w_sem.at[u, 0]
            )
        ]

    x_copy = pltpu.make_async_copy(x_hbm, x_ref, x_sem)
    x_copy.start()
    for u in range(AHEAD):
        for copy in weight_copies(u):
            copy.start()

    barrier = pltpu.get_barrier_semaphore()

    def greet(device):
        pl.semaphore_signal(barrier, inc=1, device_id=device, device_id_type=MESH)

    greet((near[1], cp))
    greet((near[2], cp))
    greet(partner)
    has_left = z > 0
    has_right = z < nz - 1
    pl.when(has_left)(lambda: greet((me, cp - 2)))
    pl.when(has_right)(lambda: greet((me, cp + 2)))

    target = slot_ref[0, 0]
    t_own[...] = jnp.full(t_own.shape, target, jnp.int32)

    start = start_ref[order_ref[target, cp]]
    start_cos, start_sin = start[0:1, :], start[1:2, :]
    cos_ref[...] = start_cos * offset_ref[0] - start_sin * offset_ref[1]
    sin_ref[...] = (start_sin * offset_ref[0] + start_cos * offset_ref[1]) * sign_ref[0:1, :]

    own_seq = seq_ref[me, cp]
    own_order = order_ref[me, cp]
    most = columns // 2
    table = []
    for i in range(most):
        index = cp
        for s in range(columns):
            hit = (seq_ref[me, s] == own_seq) & (order_ref[me, s] == i)
            index = jnp.where(hit, s, index)
        table.append(index)

    def first_bit(u):
        return 1 if u % 2 == 0 else 2

    def remote(src, dst, send, recv, device):
        return pltpu.make_async_remote_copy(
            src_ref=src, dst_ref=dst, send_sem=send, recv_sem=recv, device_id=device, device_id_type=MESH
        )

    def t_copy(bit):
        return remote(
            t_own, t_a if bit == 1 else t_b, t_send.at[bit - 1], t_recv.at[bit - 1], (near[bit], cp)
        )

    def hop1(u):
        return remote(own.at[u], recv1.at[u], s1_send.at[u], s1_recv.at[u], (near[first_bit(u)], cp))

    def hop2(u):
        return remote(
            send2.at[u], recv2.at[u], s2_send.at[u], s2_recv.at[u], (near[3 - first_bit(u)], cp)
        )

    def left_copy(g, zs):
        block = kvs[g].at[2 * zs + core]
        return remote(block, block, left_send.at[g, zs], z_recv.at[g, zs], (me, cp - 2))

    def right_copy(g, zs):
        block = kvs[g].at[2 * zs + core]
        return remote(block, block, right_send.at[g, zs], z_recv.at[g, zs], (me, cp + 2))

    def core_copy(g, zs):
        block = kvs[g].at[2 * zs + core]
        return remote(block, block, core_send.at[g, zs], core_recv.at[g, zs], partner)

    def project(u):
        for copy in weight_copies(u):
            copy.wait()
        if u + AHEAD < units:
            for copy in weight_copies(u + AHEAD):
                copy.start()
        product = jnp.dot(x_ref[...], w_ref[u], preferred_element_type=jnp.float32)
        for half in range(2):
            part = product[:, half * HD : (half + 1) * HD]
            if not (u < KVH and half == 1):
                part = part * cos_ref[...] + pltpu.roll(part, HD // 2, 1) * sin_ref[...]
            own[u, :, pl.ds(half * HD, HD)] = part.astype(jnp.bfloat16)

    def is_target(ref, device):
        return jnp.broadcast_to(ref[0:1, :] == device, (rows, HD))

    def halves(ref, u):
        return [ref[u, :, pl.ds(h * HD, HD)].astype(jnp.float32) for h in range(2)]

    def second(u):
        hop1(u).wait_recv()
        passes = is_target(t_own, near[3 - first_bit(u)])
        mine, came = halves(own, u), halves(recv1, u)
        for h in range(2):
            send2[u, :, pl.ds(h * HD, HD)] = jnp.where(passes, mine[h], came[h]).astype(jnp.bfloat16)
        hop2(u).start()

    def arrive(u):
        hop2(u).wait_recv()
        stays = is_target(t_own, me)
        first = is_target(t_a if first_bit(u) == 1 else t_b, me)
        mine, came1, came2 = halves(own, u), halves(recv1, u), halves(recv2, u)
        for h in range(2):
            value = jnp.where(stays, mine[h], jnp.where(first, came1[h], came2[h])).astype(jnp.bfloat16)
            if u < KVH:
                kvs[u][cp, :, pl.ds(h * HD, HD)] = value
            else:
                query[2 * (u - KVH) + h] = value
        if u < KVH:
            pl.when(has_left)(lambda: left_copy(u, z).start())
            pl.when(has_right)(lambda: right_copy(u, z).start())
            core_copy(u, z).start()

    def along(g, d):
        @pl.when(z + d < nz)
        def _():
            left_copy(g, z + d).wait_recv()
            pl.when(has_left)(lambda: left_copy(g, z + d).start())
            core_copy(g, z + d).start()

        @pl.when(z - d >= 0)
        def _():
            right_copy(g, z - d).wait_recv()
            pl.when(has_right)(lambda: right_copy(g, z - d).start())
            core_copy(g, z - d).start()

    def attend(g):
        for zs in range(nz):
            core_copy(g, zs).wait_recv()
        blocks = [kvs[g][index] for index in table]
        keys = jnp.concatenate([b[:, :HD] for b in blocks], axis=0)
        values = jnp.concatenate([b[:, HD:] for b in blocks], axis=0)
        heads = QH // KVH
        shape = (heads * rows, keys.shape[0])
        row_pos = lax.broadcasted_iota(jnp.int32, shape, 0) % rows + own_order * rows
        allowed = lax.broadcasted_iota(jnp.int32, shape, 1) <= row_pos
        stacked = query[pl.ds(g * heads, heads)].reshape(heads * rows, HD)
        scores = lax.dot_general(
            stacked, keys, (((1,), (1,)), ((), ())), preferred_element_type=jnp.float32
        )
        scores = jnp.where(allowed, scores, NEG_FILL)
        peak = jnp.max(scores, axis=1, keepdims=True)
        weights = jnp.exp2((scores - peak) * (HD ** -0.5 * 1.4426950408889634))
        total = jnp.sum(weights, axis=1, keepdims=True)
        mixed = jnp.dot(weights.astype(jnp.bfloat16), values, preferred_element_type=jnp.float32)
        mixed = (mixed / total).astype(jnp.bfloat16)
        for j in range(heads):
            out_ref[:, pl.ds((g * heads + j) * HD, HD)] = mixed[j * rows : (j + 1) * rows]

    x_copy.wait()
    for step in schedule(nz):
        kind, u = step[0], step[1]
        if kind == "P":
            project(u)
        elif kind == "S":
            if u == 0:
                pl.semaphore_wait(barrier, 3 + jnp.minimum(z, 1) + jnp.minimum(nz - 1 - z, 1))
                t_copy(1).start()
                t_copy(2).start()
            hop1(u).start()
        elif kind == "T":
            if u == 0:
                t_copy(1).wait()
                t_copy(2).wait()
            second(u)
        elif kind == "F":
            arrive(u)
        elif kind == "Z":
            along(u, step[2])
        else:
            attend(u)

    for u in range(units):
        hop1(u).wait_send()
        hop2(u).wait_send()
    for g in range(KVH):
        for zs in range(nz):
            core_copy(g, zs).wait_send()

            @pl.when(has_left & (z <= zs))
            def _():
                left_copy(g, zs).wait_send()

            @pl.when(has_right & (z >= zs))
            def _():
                right_copy(g, zs).wait_send()


def local(tokens, qkv_weight, owner_slot, slab_sequence, slab_order):
    loader_rows = tokens[0]
    rows, width = loader_rows.shape
    groups = lax.axis_size("dp")
    columns = lax.axis_size("cp")
    assert groups == 4 and columns % 2 == 0 and owner_slot.shape[1] == 1
    assert slab_sequence.shape[1] == columns
    nz = columns // 2
    units = (QH + 2 * KVH) * HD // UNIT
    frequency = np.float32(ROPE_BASE) ** (-np.arange(HD // 2, dtype=np.float32) * np.float32(2.0 / HD))
    frequency = np.concatenate([frequency, frequency]).astype(np.float64)
    sign = np.where(np.arange(HD) < HD // 2, -1.0, 1.0)
    starts = np.arange(columns)[:, None] * rows * frequency[None, :]
    offsets = np.arange(rows)[:, None] * frequency[None, :]
    start_table = np.stack([np.cos(starts), np.sin(starts)], axis=1).astype(np.float32)
    offset_table = np.stack([np.cos(offsets), np.sin(offsets)]).astype(np.float32)
    sign_table = np.broadcast_to(sign, (8, HD)).astype(np.float32)
    smem = pl.BlockSpec(memory_space=pltpu.SMEM)
    vmem = pl.BlockSpec(memory_space=pltpu.VMEM)
    hbm = pl.BlockSpec(memory_space=pl.ANY)
    unit_buffer = pltpu.VMEM((units, rows, UNIT), jnp.bfloat16)
    kv_buffer = pltpu.VMEM((columns, rows, UNIT), jnp.bfloat16)
    small = pltpu.VMEM((8, HD), jnp.int32)
    dma = pltpu.SemaphoreType.DMA
    context = pl.pallas_call(
        functools.partial(kernel, groups, columns),
        out_shape=jax.ShapeDtypeStruct((rows, QH * HD), jnp.bfloat16),
        in_specs=[smem, smem, smem, vmem, vmem, vmem, hbm, hbm],
        out_specs=vmem,
        scratch_shapes=[
            pltpu.VMEM((rows, width), jnp.bfloat16),
            pltpu.VMEM((units, width, UNIT), jnp.bfloat16),
            unit_buffer,
            unit_buffer,
            unit_buffer,
            unit_buffer,
            pltpu.VMEM((QH, rows, HD), jnp.bfloat16),
            kv_buffer,
            kv_buffer,
            kv_buffer,
            kv_buffer,
            small,
            small,
            small,
            pltpu.VMEM((rows, HD), jnp.float32),
            pltpu.VMEM((rows, HD), jnp.float32),
            dma,
            dma((units, 2)),
            dma((units,)),
            dma((units,)),
            dma((units,)),
            dma((units,)),
            dma((2,)),
            dma((2,)),
            dma((KVH, nz)),
            dma((KVH, nz)),
            dma((KVH, nz)),
            dma((KVH, nz)),
            dma((KVH, nz)),
        ],
        compiler_params=pltpu.CompilerParams(
            collective_id=0, has_side_effects=True, vmem_limit_bytes=60000 * 1024
        ),
    )(slab_sequence, slab_order, owner_slot, start_table, offset_table, sign_table, loader_rows, qkv_weight)
    return context[None]


def solution(mesh):
    in_specs = (P("dp", "cp", None), P(), P("dp", "cp"), P(), P())
    out_specs = P("dp", "cp", None)
    return jax.shard_map(local, mesh=mesh, in_specs=in_specs, out_specs=out_specs, check_vma=False)
```
